32 devices in a mesh: freq: 8 (over y, x, core), gz: 4 (over z).
Axes of the slice: x: 2, y: 2, z: 4, core: 2. Of those that a mesh axis runs over, the one named last changes fastest.
Arguments:
- displacement: float32 [8, 2, 3, 16, 64, 128], P('freq', None, None, 'gz'), may hold values from -6 to 6
- freq_index: int32 [8], P('freq'), may hold values from 0 to 7
- tissue: int32 [16, 64, 128], P('gz'), may hold values from 0 to 1, as said below
Outputs:
- modulus: float32 [2, 16, 64, 128], P(None, 'gz')
- residual: float32 [2, 16, 64, 128], P(None, 'gz')
The draws below stay inside these ranges and needn't reach their ends.
Inputs may be any that keep to these rules, and one draw needn't show every extreme that they name: 0 outside tissue, 1 inside; the share of tissue rises along z from about 0.15 to about 0.95.
All inputs are finite; a program needn't handle non-finite values.
Results may differ from the reference program's by a relative error of at most 0.0003.
Values sent between devices are 32-bit elements; how exact they have to be, the bound alone decides.
A program may use at most 64 MiB of HBM per device.

```python
import jax
import jax.numpy as jnp
from jax import lax

NY = 64
NX = 128
ITERS = 2
FREQ_COUNT = 8
GROUPS = 8
NZ = 16


def draw_tissue(key, part):
    depth = lax.broadcasted_iota(jnp.int32, (NZ, NY, NX), 0)
    level = 150 + 800 * depth // NZ
    rolled = jax.random.randint(key, (NZ, NY, NX), 0, 1000)
    return (rolled < level).astype(jnp.int32)


def place_ends(drawn, own_key, low, high):
    spot = [jax.random.randint(jax.random.fold_in(own_key, axis), (), 0, length) for axis, length in enumerate(drawn.shape)]
    main_axis = drawn.shape.index(max(drawn.shape))
    neighbour = spot[:main_axis] + [(spot[main_axis] + 1) % drawn.shape[main_axis]] + spot[main_axis + 1:]
    return drawn.at[tuple(spot)].set(low).at[tuple(neighbour)].set(high)


def block_levels(stream_key, dims, shards, least, largest):
    gain, own = 1.0, jax.random.fold_in(stream_key, 6)
    for position, blocks in shards:
        steps = jnp.exp(jax.random.uniform(jax.random.fold_in(own, position), (blocks,), jnp.float32, least / len(shards), largest / len(shards)))
        gain = gain * jnp.repeat(steps, dims[position] // blocks).reshape([-1 if axis == position else 1 for axis in range(len(dims))])
    return gain


def noise(rng, dims, deviation, bound, shards=(), kind=jnp.bfloat16):
    entries = deviation * jax.random.normal(rng, dims, jnp.float32)
    if shards:
        entries = entries * block_levels(rng, dims, shards, -0.22, 0.18)
    return jnp.clip(entries, -bound, bound).astype(kind)


def setup_inputs(seed: int = 0) -> dict:
    key_list = jax.random.split(jax.random.key(seed), 4)
    return {
        "displacement": noise(key_list[0], (GROUPS, 2, 3, NZ, NY, NX), 1.0, 6.0, ((0, 8), (3, 4)), jnp.float32),
        "freq_index": place_ends(jax.random.randint(key_list[1], (GROUPS,), 0, FREQ_COUNT), jax.random.fold_in(key_list[1], 1), 0, FREQ_COUNT - 1).astype(jnp.int32),
        "tissue": draw_tissue(jax.random.fold_in(key_list[3], 71), 0),
    }


DAMPING = 0.05


def zero_plane(field, spatial):
    return jnp.zeros_like(lax.slice_in_dim(field, 0, 1, axis=spatial))


def ahead(field, spatial, tail):
    moved = lax.slice_in_dim(field, 1, field.shape[spatial], axis=spatial)
    return jnp.concatenate([moved, tail], axis=spatial)


def behind(field, spatial, head):
    moved = lax.slice_in_dim(field, 0, field.shape[spatial] - 1, axis=spatial)
    return jnp.concatenate([head, moved], axis=spatial)


def gradients(field):
    return [ahead(field, spatial, zero_plane(field, spatial)) - field for spatial in (2, 3, 4)]


def forward(modulus, grads):
    total = None
    for spatial, grad in zip((2, 3, 4), grads):
        real = modulus[0] * grad[0] - modulus[1] * grad[1]
        imag = modulus[0] * grad[1] + modulus[1] * grad[0]
        flux = jnp.stack([real, imag])
        term = flux - behind(flux, spatial, zero_plane(flux, spatial))
        total = term if total is None else total + term
    return total


def adjoint(values, grads):
    real = None
    imag = None
    for spatial, grad in zip((2, 3, 4), grads):
        diff = values - ahead(values, spatial, zero_plane(values, spatial))
        part_real = jnp.sum(grad[0] * diff[0] + grad[1] * diff[1], axis=0)
        part_imag = jnp.sum(grad[0] * diff[1] - grad[1] * diff[0], axis=0)
        real = part_real if real is None else real + part_real
        imag = part_imag if imag is None else imag + part_imag
    return jnp.stack([real, imag])


def reference(displacement, freq_index, tissue):
    weight = tissue.astype(jnp.float32)
    empty = jnp.zeros((2, NZ, NY, NX), jnp.float32)

    def right_group(carry, item):
        field, index = item
        grads = gradients(field)
        kappa = 0.2 * (index + 1).astype(jnp.float32)
        return carry + adjoint(weight * (-kappa * field), grads), None

    def normal_apply(direction):
        def one_group(carry, item):
            field, index = item
            grads = gradients(field)
            return carry + adjoint(weight * forward(direction, grads), grads), None

        total, _ = lax.scan(one_group, empty, (displacement, freq_index))
        return total + DAMPING * direction

    right, _ = lax.scan(right_group, empty, (displacement, freq_index))
    modulus = empty
    residual = right
    direction = right
    norm_now = jnp.sum(residual * residual)
    for iteration in range(ITERS):
        image = normal_apply(direction)
        step_size = norm_now / jnp.sum(direction * image)
        modulus = modulus + step_size * direction
        residual = residual - step_size * image
        norm_next = jnp.sum(residual * residual)
        direction = residual + (norm_next / norm_now) * direction
        norm_now = norm_next
    return modulus, residual
```

```python
import functools

import jax
import jax.numpy as jnp
from jax import lax
from jax.experimental import pallas as pl
from jax.experimental.pallas import tpu as pltpu
from jax.sharding import PartitionSpec as P

MESH = pl.DeviceIdType.MESH
DAMPING = 0.05
ZZ, Z0, ZY, ZX = 0, 1, 3, 5
YY, Y0, YX = 7, 8, 10
CC, C0X, XX = 12, 13, 15
FIELDS = 16


def shifted_up(array, tail):
    rows = array.shape[0]
    if rows % 8 == 0:
        last = lax.broadcasted_iota(jnp.int32, array.shape, 0) == rows - 1
        return jnp.where(last, jnp.broadcast_to(tail, array.shape), pltpu.roll(array, rows - 1, 0))
    return jnp.concatenate([array[1:], tail], axis=0)


def shifted_down(array, head):
    rows = array.shape[0]
    if rows % 8 == 0:
        first = lax.broadcasted_iota(jnp.int32, array.shape, 0) == 0
        return jnp.where(first, jnp.broadcast_to(head, array.shape), pltpu.roll(array, 1, 0))
    return jnp.concatenate([head, array[:-1]], axis=0)


def lane_next(array):
    return pltpu.roll(array, array.shape[1] - 1, 1)


def lane_prev(array):
    return pltpu.roll(array, 1, 1)


def mul(a, b):
    return a[0] * b[0] - a[1] * b[1], a[0] * b[1] + a[1] * b[0]


def cmul(a, b):
    return a[0] * b[0] + a[1] * b[1], a[0] * b[1] - a[1] * b[0]


def add(*terms):
    return sum(t[0] for t in terms[1:]) + terms[0][0], sum(t[1] for t in terms[1:]) + terms[0][1]


def scale(r, a):
    return r * a[0], r * a[1]


def kernel(nf, nz, u, tis, fi, mod_out, res_out,
           ubuf, hsrc, hbuf, zlo, zhi, wsrc, wz, macc, bacc, mz, ysrc, yp, gath, mlo, mloc, mhi, mhic,
           scs, scr, sgs, sgr,
           loc_s, main_s, main_r, halo_s, halo_r, flo_s, fhi_s, zlo_r, zhi_r, w_sem, mz_sem, yp_sem,
           ag_s, ag_r, pl_s, pl_r, sc_s, sc_r, sg_s, sg_r):
    f = lax.axis_index("freq")
    z = lax.axis_index("gz")
    _, comps, depth, _, rows, width = u.shape
    below, above = z > 0, z < nz - 1
    first, last = f > 0, f < nf - 1
    fnext, fprev = lax.rem(f + 1, nf), lax.rem(f + nf - 1, nf)
    zn, zp = z + 1, z - 1

    def remote(src, dst, ssem, rsem, df, dz):
        return pltpu.make_async_remote_copy(
            src_ref=src, dst_ref=dst, send_sem=ssem, recv_sem=rsem, device_id=(df, dz), device_id_type=MESH)

    barrier = pltpu.get_barrier_semaphore()

    def greet(df, dz):
        pl.semaphore_signal(barrier, inc=1, device_id=(df, dz), device_id_type=MESH)

    for k in range(1, nf):
        greet(lax.rem(f + k, nf), z)
    for k in range(1, nz):
        greet(f, lax.rem(z + k, nz))
    diag_up = jnp.logical_and(first, above)
    diag_down = jnp.logical_and(last, below)

    @pl.when(diag_up)
    def _():
        greet(f - 1, zn)

    @pl.when(diag_down)
    def _():
        greet(f + 1, zp)

    kappa = 0.2 * (fi[0] + 1).astype(jnp.float32)
    zero_row = jnp.zeros((1, width), jnp.float32)
    for d in range(nf):
        for p in range(2):
            for c in range(comps):
                for i in range(depth):
                    lo = u[p, c, i, d - 1, rows - 1:rows, :] if d > 0 else zero_row
                    hi = u[p, c, i, d + 1, 0:1, :] if d < nf - 1 else zero_row
                    hsrc[d, p * comps + c, i:i + 1, :] = lo
                    hsrc[d, p * comps + c, depth + i:depth + i + 1, :] = hi
        hsrc[d, 2 * comps] = jnp.full((2 * depth, width), kappa, jnp.float32)
    wsrc[...] = tis[0, f].astype(jnp.float32)

    @pl.when(jnp.logical_not(below))
    def _():
        zlo[...] = jnp.zeros_like(zlo)
        mlo[...] = jnp.zeros_like(mlo)

    @pl.when(jnp.logical_not(above))
    def _():
        zhi[...] = jnp.zeros_like(zhi)
        mhi[...] = jnp.zeros_like(mhi)
        wz[...] = jnp.zeros_like(wz)
        mz[...] = jnp.zeros_like(mz)

    @pl.when(jnp.logical_not(last))
    def _():
        yp[...] = jnp.zeros_like(yp)

    @pl.when(jnp.logical_not(diag_up))
    def _():
        mhic[...] = jnp.zeros_like(mhic)

    @pl.when(jnp.logical_not(diag_down))
    def _():
        mloc[...] = jnp.zeros_like(mloc)

    own_u = pltpu.make_async_copy(u.at[:, :, :, f], ubuf.at[f], loc_s.at[0])
    own_h = pltpu.make_async_copy(hsrc.at[f], hbuf.at[f], loc_s.at[1])
    own_u.start()
    own_h.start()
    macc[...] = jnp.zeros_like(macc)
    bacc[...] = jnp.zeros_like(bacc)

    pl.semaphore_wait(barrier, (nf - 1) + (nz - 1) + diag_up.astype(jnp.int32) + diag_down.astype(jnp.int32))

    def sends(d):
        return (remote(hsrc.at[d], hbuf.at[f], halo_s.at[d], halo_r.at[f], d, z),
                remote(u.at[:, :, :, d], ubuf.at[f], main_s.at[d], main_r.at[f], d, z))

    def arrivals(s):
        return (remote(hsrc.at[s], hbuf.at[s], halo_s.at[s], halo_r.at[s], s, z),
                remote(u.at[:, :, :, s], ubuf.at[s], main_s.at[s], main_r.at[s], s, z))

    for k in range(1, nf):
        for copy in sends(lax.rem(f + k, nf)):
            copy.start()

    w_copy = remote(wsrc, wz, w_sem.at[0], w_sem.at[1], f, zp)
    w_from = remote(wsrc, wz, w_sem.at[0], w_sem.at[1], f, zn)

    @pl.when(below)
    def _():
        w_copy.start()

    def forward_up(s):
        return remote(ubuf.at[s, :, :, depth - 1], zlo.at[s], flo_s.at[s], zlo_r.at[s], f, zn)

    def forward_down(s):
        return remote(ubuf.at[s, :, :, 0], zhi.at[s], fhi_s.at[s], zhi_r.at[s], f, zp)

    def from_below(s):
        return remote(ubuf.at[s, :, :, depth - 1], zlo.at[s], flo_s.at[s], zlo_r.at[s], f, zp)

    def from_above(s):
        return remote(ubuf.at[s, :, :, 0], zhi.at[s], fhi_s.at[s], zhi_r.at[s], f, zn)

    def forwards(s):
        @pl.when(above)
        def _():
            forward_up(s).start()

        @pl.when(below)
        def _():
            forward_down(s).start()

    own_u.wait()
    own_h.wait()
    forwards(f)

    @pl.when(above)
    def _():
        w_from.wait_recv()

    lane_last = lax.broadcasted_iota(jnp.int32, (rows, width), 1) == width - 1
    lane_first = lax.broadcasted_iota(jnp.int32, (rows, width), 1) == 0
    last_scale = jnp.where(last, 1.0, 0.0).astype(jnp.float32)

    def weight(i):
        return tis[i, f].astype(jnp.float32)

    def group(s):
        kap = hbuf[s, 2 * comps, 0:1, :]
        for i in range(depth):
            w = weight(i)
            w_z = weight(i + 1) if i + 1 < depth else wz[...]
            w_y = shifted_up(w, tis[i, fnext, 0:1, :].astype(jnp.float32) * last_scale)
            w_x = jnp.where(lane_last, 0.0, lane_next(w))
            tot = [None] * FIELDS
            right = None
            for c in range(comps):
                here, az, ay, ax, gz, gy, gx, uz, uy, ux = ([None, None] for _ in range(10))
                for p in range(2):
                    v = ubuf[s, p, c, i]
                    prev_z = ubuf[s, p, c, i - 1] if i > 0 else zlo[s, p, c]
                    next_z = ubuf[s, p, c, i + 1] if i + 1 < depth else zhi[s, p, c]
                    lo = hbuf[s, p * comps + c, i:i + 1, :]
                    hi = hbuf[s, p * comps + c, depth + i:depth + i + 1, :]
                    next_y = shifted_up(v, hi)
                    prev_y = shifted_down(v, lo)
                    next_x = jnp.where(lane_last, 0.0, lane_next(v))
                    prev_x = lane_prev(v)
                    here[p] = v
                    uz[p], uy[p], ux[p] = next_z, next_y, next_x
                    gz[p], gy[p], gx[p] = next_z - v, next_y - v, next_x - v
                    az[p], ay[p], ax[p] = v - prev_z, v - prev_y, v - prev_x
                h = [-(gz[p] + gy[p] + gx[p]) for p in range(2)]
                parts = [None] * FIELDS
                parts[ZZ] = az[0] * az[0] + az[1] * az[1]
                parts[YY] = ay[0] * ay[0] + ay[1] * ay[1]
                parts[XX] = ax[0] * ax[0] + ax[1] * ax[1]
                parts[CC] = h[0] * h[0] + h[1] * h[1]
                parts[Z0:Z0 + 2] = cmul(az, h)
                parts[ZY:ZY + 2] = cmul(az, ay)
                parts[ZX:ZX + 2] = cmul(az, ax)
                parts[Y0:Y0 + 2] = cmul(ay, h)
                parts[YX:YX + 2] = cmul(ay, ax)
                parts[C0X:C0X + 2] = cmul(h, ax)
                tot = parts if c == 0 else [a + b for a, b in zip(tot, parts)]
                t = [w * here[p] for p in range(2)]
                for g, wn, un in ((gz, w_z, uz), (gy, w_y, uy), (gx, w_x, ux)):
                    term = cmul(g, [t[p] - wn * un[p] for p in range(2)])
                    right = term if right is None else add(right, term)
            for n in range(FIELDS):
                macc[n, i] += tot[n]
            for p in range(2):
                bacc[p, i] += kap * right[p]

    def z_ready(s):
        @pl.when(below)
        def _():
            from_below(s).wait_recv()

        @pl.when(above)
        def _():
            from_above(s).wait_recv()

    def step(k, carry):
        s = lax.rem(f - k + nf, nf)
        before = lax.rem(f - k + 1 + nf, nf)
        for copy in arrivals(s):
            copy.wait_recv()
        forwards(s)
        z_ready(before)
        group(before)
        return carry

    lax.fori_loop(1, nf, step, 0)
    z_ready(fnext)
    group(fnext)

    for i in range(depth):
        for p in range(2):
            gath[0, f, p, i] = -bacc[p, i]

    def plane_sends(t):
        own = gath.at[t, f]
        return ((above, remote(own.at[:, depth - 1], mlo.at[t], pl_s.at[t, 0], pl_r.at[t, 0], f, zn)),
                (below, remote(own.at[:, 0], mhi.at[t], pl_s.at[t, 1], pl_r.at[t, 1], f, zp)),
                (diag_up, remote(own.at[:, depth - 1], mloc.at[t], pl_s.at[t, 2], pl_r.at[t, 2], f - 1, zn)),
                (diag_down, remote(own.at[:, 0], mhic.at[t], pl_s.at[t, 3], pl_r.at[t, 3], f + 1, zp)))

    def plane_arrivals(t):
        own = gath.at[t, f]
        return ((below, remote(own.at[:, depth - 1], mlo.at[t], pl_s.at[t, 0], pl_r.at[t, 0], f, zp)),
                (above, remote(own.at[:, 0], mhi.at[t], pl_s.at[t, 1], pl_r.at[t, 1], f, zn)),
                (diag_down, remote(own.at[:, depth - 1], mloc.at[t], pl_s.at[t, 2], pl_r.at[t, 2], f + 1, zp)),
                (diag_up, remote(own.at[:, 0], mhic.at[t], pl_s.at[t, 3], pl_r.at[t, 3], f - 1, zn)))

    def started(pairs):
        for cond, copy in pairs:
            pl.when(cond)(copy.start)

    def received(pairs):
        for cond, copy in pairs:
            pl.when(cond)(copy.wait_recv)

    def sent(pairs):
        for cond, copy in pairs:
            pl.when(cond)(copy.wait_send)

    order = []
    for k in range(1, nf // 2 + 1):
        order.append(k)
        if nf - k != k:
            order.append(nf - k)

    def tile_send(t, k):
        return remote(gath.at[t, f], gath.at[t, f], ag_s.at[t, k], ag_r.at[t, f], lax.rem(f + k, nf), z)

    def tile_from(t, s):
        return remote(gath.at[t, s], gath.at[t, s], ag_s.at[t, 0], ag_r.at[t, s], s, z)

    started(plane_sends(0))
    for k in order[:2]:
        tile_send(0, k).start()

    y_first = jnp.logical_and(lax.broadcasted_iota(jnp.int32, (rows, width), 0) == 0, f == 0)
    for i in range(depth):
        w = weight(i)
        zm = w * jnp.where(below, 1.0, 0.0).astype(jnp.float32) if i == 0 else w
        for n in range(FIELDS):
            val = macc[n, i] * (zm if n < YY else w)
            if n in (YY, Y0, Y0 + 1, YX, YX + 1, ZY, ZY + 1):
                val = jnp.where(y_first, 0.0, val)
            if n in (XX, ZX, ZX + 1, YX, YX + 1, C0X, C0X + 1):
                val = jnp.where(lane_first, 0.0, val)
            macc[n, i] = val
            if n in (ZY, ZY + 1):
                ysrc[5 + n - ZY, i:i + 1, :] = val[0:1]
            elif YY <= n < CC:
                ysrc[n - YY, i:i + 1, :] = val[0:1]

    mz_pair = ((below, remote(macc.at[0:YY, 0], mz, mz_sem.at[0], mz_sem.at[1], f, zp)),)
    mz_from = ((above, remote(macc.at[0:YY, 0], mz, mz_sem.at[0], mz_sem.at[1], f, zn)),)
    yp_pair = ((first, remote(ysrc, yp, yp_sem.at[0], yp_sem.at[1], fprev, z)),)
    yp_from = ((last, remote(ysrc, yp, yp_sem.at[0], yp_sem.at[1], fnext, z)),)
    started(mz_pair)
    started(yp_pair)
    for k in order[2:]:
        tile_send(0, k).start()

    def apply(t):
        rows_next = [gath[t, fnext, p, :, 0, :] for p in range(2)]
        rows_here = [gath[t, f, p, :, rows - 1, :] for p in range(2)]
        rows_z = [jnp.concatenate([mloc[t, p, 0:1, :], rows_next[p][:-1]], axis=0) for p in range(2)]
        rows_x = [lane_prev(rows_next[p]) for p in range(2)]
        vy_edge = add(scale(yp[0], rows_here), mul((yp[1], yp[2]), rows_next), mul((yp[3], yp[4]), rows_x),
                      cmul((yp[5], yp[6]), rows_z))
        m4 = [mhi[t, p] for p in range(2)]
        m4y = [shifted_down(m4[p], mhic[t, p, rows - 1:rows, :]) for p in range(2)]
        m4x = [lane_prev(m4[p]) for p in range(2)]
        m4z = [gath[t, f, p, depth - 1] for p in range(2)]
        vz_edge = add(scale(mz[ZZ], m4z), mul((mz[Z0], mz[Z0 + 1]), m4), mul((mz[ZY], mz[ZY + 1]), m4y),
                      mul((mz[ZX], mz[ZX + 1]), m4x))
        after = vz_edge
        for i in reversed(range(depth)):
            m = [gath[t, f, p, i] for p in range(2)]
            m_z = [gath[t, f, p, i - 1] if i > 0 else mlo[t, p] for p in range(2)]
            m_y = [shifted_down(m[p], gath[t, fprev, p, i, rows - 1:rows, :]) for p in range(2)]
            m_x = [lane_prev(m[p]) for p in range(2)]

            def pair(n):
                return macc[n, i], macc[n + 1, i]

            z0, zy, zx, y0, yx, cx = pair(Z0), pair(ZY), pair(ZX), pair(Y0), pair(YX), pair(C0X)
            v0 = add(scale(macc[CC, i], m), cmul(z0, m_z), cmul(y0, m_y), mul(cx, m_x))
            vx = add(scale(macc[XX, i], m_x), cmul(cx, m), cmul(zx, m_z), cmul(yx, m_y))
            vy = add(scale(macc[YY, i], m_y), mul(y0, m), mul(yx, m_x), cmul(zy, m_z))
            vz = add(scale(macc[ZZ, i], m_z), mul(z0, m), mul(zy, m_y), mul(zx, m_x))
            for p in range(2):
                gath[t + 1, f, p, i] = (v0[p] + lane_next(vx[p]) + shifted_up(vy[p], vy_edge[p][i:i + 1])
                                        + after[p] + DAMPING * m[p])
            after = vz

    def halo_ready(t):
        received(plane_arrivals(t))
        tile_from(t, fnext).wait_recv()
        tile_from(t, fprev).wait_recv()

    received(mz_from)
    received(yp_from)
    halo_ready(0)
    apply(0)
    started(plane_sends(1))
    for k in order:
        tile_send(1, k).start()

    def product(a, b):
        total = None
        for i in range(depth):
            for p in range(2):
                term = gath[a, f, p, i] * gath[b, f, p, i]
                total = term if total is None else total + term
        return jnp.sum(total, axis=0, keepdims=True)

    scs[0, 0:1, :] = product(0, 0)
    scs[0, 1:2, :] = product(0, 1)
    scs[0, 2:3, :] = product(1, 1)
    halo_ready(1)
    apply(1)
    scs[0, 3:4, :] = product(1, 2)

    def part_send(k):
        return remote(scs.at[0], scr.at[f], sc_s.at[k], sc_r.at[f], lax.rem(f + k, nf), z)

    for k in order:
        part_send(k).start()
    for k in order:
        tile_send(2, k).start()
    total = scs[0]
    for k in order:
        s = lax.rem(f - k + nf, nf)
        remote(scs.at[0], scr.at[s], sc_s.at[k], sc_r.at[s], s, z).wait_recv()
        total = total + scr[s]
    sgs[0] = total

    def sum_send(k):
        return remote(sgs.at[0], sgr.at[z], sg_s.at[k], sg_r.at[z], f, lax.rem(z + k, nz))

    for k in range(1, nz):
        sum_send(k).start()
    for k in range(1, nz):
        s = lax.rem(z - k + nz, nz)
        remote(sgs.at[0], sgr.at[s], sg_s.at[k], sg_r.at[s], f, s).wait_recv()
        total = total + sgr[s]
    sums = jnp.sum(total, axis=1, keepdims=True)
    bb, bq, qq, qs = (sums[n:n + 1, :] for n in range(4))
    alpha = bb / bq
    norm = bb - 2.0 * alpha * bq + alpha * alpha * qq
    beta = 1.0 + norm / bb
    second = norm / (beta * beta * bq - 2.0 * alpha * beta * qq + alpha * alpha * qs)
    c1 = jnp.broadcast_to(alpha + second * beta, (rows, width))
    c2 = jnp.broadcast_to(alpha * second, (rows, width))

    def finish(s):
        for p in range(2):
            for i in range(depth):
                b, q, r = gath[0, s, p, i], gath[1, s, p, i], gath[2, s, p, i]
                mod_out[p, i, s] = c1 * b - c2 * q
                res_out[p, i, s] = b - c1 * q + c2 * r

    finish(f)
    for k in order:
        s = lax.rem(f - k + nf, nf)
        if k not in (1, nf - 1):
            tile_from(0, s).wait_recv()
            tile_from(1, s).wait_recv()
        tile_from(2, s).wait_recv()
        finish(s)

    for k in range(1, nf):
        for copy in sends(lax.rem(f + k, nf)):
            copy.wait_send()
        for t in range(3):
            tile_send(t, k).wait_send()
        part_send(k).wait_send()
    for s in range(nf):
        pl.when(above)(forward_up(s).wait_send)
        pl.when(below)(forward_down(s).wait_send)
    pl.when(below)(w_copy.wait_send)
    sent(mz_pair)
    sent(yp_pair)
    for t in range(2):
        sent(plane_sends(t))
    for k in range(1, nz):
        sum_send(k).wait_send()


def body(nf, nz, displacement, freq_index, tissue):
    _, _, comps, depth, height, width = displacement.shape
    rows = height // nf
    u = displacement.reshape(2, comps, depth, nf, rows, width)
    tis = tissue.reshape(depth, nf, rows, width)
    f32 = jnp.float32
    dma = pltpu.SemaphoreType.DMA
    vmem = pl.BlockSpec(memory_space=pltpu.VMEM)
    out = jax.ShapeDtypeStruct((2, depth, nf, rows, width), f32)
    modulus, residual = pl.pallas_call(
        functools.partial(kernel, nf, nz),
        out_shape=(out, out),
        in_specs=[vmem, vmem, pl.BlockSpec(memory_space=pltpu.SMEM)],
        out_specs=(vmem, vmem),
        scratch_shapes=[
            pltpu.VMEM((nf, 2, comps, depth, rows, width), f32),
            pltpu.VMEM((nf, 2 * comps + 1, 2 * depth, width), f32),
            pltpu.VMEM((nf, 2 * comps + 1, 2 * depth, width), f32),
            pltpu.VMEM((nf, 2, comps, rows, width), f32),
            pltpu.VMEM((nf, 2, comps, rows, width), f32),
            pltpu.VMEM((rows, width), f32),
            pltpu.VMEM((rows, width), f32),
            pltpu.VMEM((FIELDS, depth, rows, width), f32),
            pltpu.VMEM((2, depth, rows, width), f32),
            pltpu.VMEM((YY, rows, width), f32),
            pltpu.VMEM((7, depth, width), f32),
            pltpu.VMEM((7, depth, width), f32),
            pltpu.VMEM((3, nf, 2, depth, rows, width), f32),
            pltpu.VMEM((2, 2, rows, width), f32),
            pltpu.VMEM((2, 2, rows, width), f32),
            pltpu.VMEM((2, 2, rows, width), f32),
            pltpu.VMEM((2, 2, rows, width), f32),
            pltpu.VMEM((1, 4, width), f32),
            pltpu.VMEM((nf, 4, width), f32),
            pltpu.VMEM((1, 4, width), f32),
            pltpu.VMEM((nz, 4, width), f32),
            dma((2,)), dma((nf,)), dma((nf,)), dma((nf,)), dma((nf,)),
            dma((nf,)), dma((nf,)), dma((nf,)), dma((nf,)),
            dma((2,)), dma((2,)), dma((2,)),
            dma((3, nf)), dma((3, nf)), dma((2, 4)), dma((2, 4)),
            dma((nf,)), dma((nf,)), dma((nz,)), dma((nz,)),
        ],
        compiler_params=pltpu.CompilerParams(collective_id=0, has_side_effects=True),
    )(u, tis, freq_index)
    shape = (2, depth, height, width)
    return modulus.reshape(shape), residual.reshape(shape)


def solution(mesh):
    placed = (P("freq", None, None, "gz", None, None), P("freq"), P("gz", None, None))
    return jax.shard_map(
        functools.partial(body, mesh.shape["freq"], mesh.shape["gz"]),
        mesh=mesh,
        in_specs=placed,
        out_specs=(P(None, "gz", None, None), P(None, "gz", None, None)),
        check_vma=False,
    )
```

```python
import functools

import jax
import jax.numpy as jnp
from jax import lax
from jax.experimental import pallas as pl
from jax.experimental.pallas import tpu as pltpu
from jax.sharding import PartitionSpec as P

MESH = pl.DeviceIdType.MESH
DAMPING = 0.05
ZZ, Z0, ZY, ZX = 0, 1, 3, 5
YY, Y0, YX = 7, 8, 10
CC, C0X, XX = 12, 13, 15
FIELDS = 16


def shifted_up(array, tail):
    rows = array.shape[0]
    if rows % 8 == 0:
        last = lax.broadcasted_iota(jnp.int32, array.shape, 0) == rows - 1
        return jnp.where(last, jnp.broadcast_to(tail, array.shape), pltpu.roll(array, rows - 1, 0))
    return jnp.concatenate([array[1:], tail], axis=0)


def shifted_down(array, head):
    rows = array.shape[0]
    if rows % 8 == 0:
        first = lax.broadcasted_iota(jnp.int32, array.shape, 0) == 0
        return jnp.where(first, jnp.broadcast_to(head, array.shape), pltpu.roll(array, 1, 0))
    return jnp.concatenate([head, array[:-1]], axis=0)


def lane_next(array):
    return pltpu.roll(array, array.shape[1] - 1, 1)


def lane_prev(array):
    return pltpu.roll(array, 1, 1)


def mul(a, b):
    return a[0] * b[0] - a[1] * b[1], a[0] * b[1] + a[1] * b[0]


def cmul(a, b):
    return a[0] * b[0] + a[1] * b[1], a[0] * b[1] - a[1] * b[0]


def add(*terms):
    return sum(t[0] for t in terms[1:]) + terms[0][0], sum(t[1] for t in terms[1:]) + terms[0][1]


def scale(r, a):
    return r * a[0], r * a[1]


def kernel(nf, nz, u, tis, fi, mod_out, res_out,
           ubuf, hsrc, hbuf, zlo, zhi, wsrc, wz, macc, bacc, mz, ysrc, yp, gath, mlo, mloc, mhi, mhic,
           scs, scr, sgs, sgr,
           loc_s, main_s, main_r, halo_s, halo_r, flo_s, fhi_s, zlo_r, zhi_r, w_sem, mz_sem, yp_sem,
           ag_s, ag_r, pl_s, pl_r, sc_s, sc_r, sg_s, sg_r):
    f = lax.axis_index("freq")
    z = lax.axis_index("gz")
    _, comps, depth, _, rows, width = u.shape
    below, above = z > 0, z < nz - 1
    first, last = f > 0, f < nf - 1
    fnext, fprev = lax.rem(f + 1, nf), lax.rem(f + nf - 1, nf)
    zn, zp = z + 1, z - 1

    def remote(src, dst, ssem, rsem, df, dz):
        return pltpu.make_async_remote_copy(
            src_ref=src, dst_ref=dst, send_sem=ssem, recv_sem=rsem, device_id=(df, dz), device_id_type=MESH)

    barrier = pltpu.get_barrier_semaphore()

    def greet(df, dz):
        pl.semaphore_signal(barrier, inc=1, device_id=(df, dz), device_id_type=MESH)

    for k in range(1, nf):
        greet(lax.rem(f + k, nf), z)
    for k in range(1, nz):
        greet(f, lax.rem(z + k, nz))
    diag_up = jnp.logical_and(first, above)
    diag_down = jnp.logical_and(last, below)

    @pl.when(diag_up)
    def _():
        greet(f - 1, zn)

    @pl.when(diag_down)
    def _():
        greet(f + 1, zp)

    kappa = 0.2 * (fi[0] + 1).astype(jnp.float32)
    zero_row = jnp.zeros((1, width), jnp.float32)
    for d in range(nf):
        for p in range(2):
            for c in range(comps):
                for i in range(depth):
                    lo = u[p, c, i, d - 1, rows - 1:rows, :] if d > 0 else zero_row
                    hi = u[p, c, i, d + 1, 0:1, :] if d < nf - 1 else zero_row
                    hsrc[d, p * comps + c, i:i + 1, :] = lo
                    hsrc[d, p * comps + c, depth + i:depth + i + 1, :] = hi
        hsrc[d, 2 * comps] = jnp.full((2 * depth, width), kappa, jnp.float32)
    wsrc[...] = tis[0, f].astype(jnp.float32)

    @pl.when(jnp.logical_not(below))
    def _():
        zlo[...] = jnp.zeros_like(zlo)
        mlo[...] = jnp.zeros_like(mlo)

    @pl.when(jnp.logical_not(above))
    def _():
        zhi[...] = jnp.zeros_like(zhi)
        mhi[...] = jnp.zeros_like(mhi)
        wz[...] = jnp.zeros_like(wz)
        mz[...] = jnp.zeros_like(mz)

    @pl.when(jnp.logical_not(last))
    def _():
        yp[...] = jnp.zeros_like(yp)

    @pl.when(jnp.logical_not(diag_up))
    def _():
        mhic[...] = jnp.zeros_like(mhic)

    @pl.when(jnp.logical_not(diag_down))
    def _():
        mloc[...] = jnp.zeros_like(mloc)

    own_u = pltpu.make_async_copy(u.at[:, :, :, f], ubuf.at[f], loc_s.at[0])
    own_h = pltpu.make_async_copy(hsrc.at[f], hbuf.at[f], loc_s.at[1])
    own_u.start()
    own_h.start()
    macc[...] = jnp.zeros_like(macc)
    bacc[...] = jnp.zeros_like(bacc)

    pl.semaphore_wait(barrier, (nf - 1) + (nz - 1) + diag_up.astype(jnp.int32) + diag_down.astype(jnp.int32))

    order = []
    for k in range(1, nf // 2 + 1):
        order.append(k)
        if nf - k != k:
            order.append(nf - k)

    def sends(d):
        return (remote(hsrc.at[d], hbuf.at[f], halo_s.at[d], halo_r.at[f], d, z),
                remote(u.at[:, :, :, d], ubuf.at[f], main_s.at[d], main_r.at[f], d, z))

    def arrivals(s):
        return (remote(hsrc.at[s], hbuf.at[s], halo_s.at[s], halo_r.at[s], s, z),
                remote(u.at[:, :, :, s], ubuf.at[s], main_s.at[s], main_r.at[s], s, z))

    for part in (1, 0):
        for k in order:
            sends(lax.rem(f + k, nf))[part].start()

    w_copy = remote(wsrc, wz, w_sem.at[0], w_sem.at[1], f, zp)
    w_from = remote(wsrc, wz, w_sem.at[0], w_sem.at[1], f, zn)

    @pl.when(below)
    def _():
        w_copy.start()

    def forward_up(s):
        return remote(ubuf.at[s, :, :, depth - 1], zlo.at[s], flo_s.at[s], zlo_r.at[s], f, zn)

    def forward_down(s):
        return remote(ubuf.at[s, :, :, 0], zhi.at[s], fhi_s.at[s], zhi_r.at[s], f, zp)

    def from_below(s):
        return remote(ubuf.at[s, :, :, depth - 1], zlo.at[s], flo_s.at[s], zlo_r.at[s], f, zp)

    def from_above(s):
        return remote(ubuf.at[s, :, :, 0], zhi.at[s], fhi_s.at[s], zhi_r.at[s], f, zn)

    def forwards(s):
        @pl.when(above)
        def _():
            forward_up(s).start()

        @pl.when(below)
        def _():
            forward_down(s).start()

    own_u.wait()
    own_h.wait()
    forwards(f)

    @pl.when(above)
    def _():
        w_from.wait_recv()

    lane_last = lax.broadcasted_iota(jnp.int32, (rows, width), 1) == width - 1
    lane_first = lax.broadcasted_iota(jnp.int32, (rows, width), 1) == 0
    last_scale = jnp.where(last, 1.0, 0.0).astype(jnp.float32)

    def weight(i):
        return tis[i, f].astype(jnp.float32)

    def group(s):
        kap = hbuf[s, 2 * comps, 0:1, :]
        for i in range(depth):
            w = weight(i)
            w_z = weight(i + 1) if i + 1 < depth else wz[...]
            w_y = shifted_up(w, tis[i, fnext, 0:1, :].astype(jnp.float32) * last_scale)
            w_x = jnp.where(lane_last, 0.0, lane_next(w))
            tot = [None] * FIELDS
            right = None
            for c in range(comps):
                here, az, ay, ax, gz, gy, gx, uz, uy, ux = ([None, None] for _ in range(10))
                for p in range(2):
                    v = ubuf[s, p, c, i]
                    prev_z = ubuf[s, p, c, i - 1] if i > 0 else zlo[s, p, c]
                    next_z = ubuf[s, p, c, i + 1] if i + 1 < depth else zhi[s, p, c]
                    lo = hbuf[s, p * comps + c, i:i + 1, :]
                    hi = hbuf[s, p * comps + c, depth + i:depth + i + 1, :]
                    next_y = shifted_up(v, hi)
                    prev_y = shifted_down(v, lo)
                    next_x = jnp.where(lane_last, 0.0, lane_next(v))
                    prev_x = lane_prev(v)
                    here[p] = v
                    uz[p], uy[p], ux[p] = next_z, next_y, next_x
                    gz[p], gy[p], gx[p] = next_z - v, next_y - v, next_x - v
                    az[p], ay[p], ax[p] = v - prev_z, v - prev_y, v - prev_x
                h = [-(gz[p] + gy[p] + gx[p]) for p in range(2)]
                parts = [None] * FIELDS
                parts[ZZ] = az[0] * az[0] + az[1] * az[1]
                parts[YY] = ay[0] * ay[0] + ay[1] * ay[1]
                parts[XX] = ax[0] * ax[0] + ax[1] * ax[1]
                parts[CC] = h[0] * h[0] + h[1] * h[1]
                parts[Z0:Z0 + 2] = cmul(az, h)
                parts[ZY:ZY + 2] = cmul(az, ay)
                parts[ZX:ZX + 2] = cmul(az, ax)
                parts[Y0:Y0 + 2] = cmul(ay, h)
                parts[YX:YX + 2] = cmul(ay, ax)
                parts[C0X:C0X + 2] = cmul(h, ax)
                tot = parts if c == 0 else [a + b for a, b in zip(tot, parts)]
                t = [w * here[p] for p in range(2)]
                for g, wn, un in ((gz, w_z, uz), (gy, w_y, uy), (gx, w_x, ux)):
                    term = cmul(g, [t[p] - wn * un[p] for p in range(2)])
                    right = term if right is None else add(right, term)
            for n in range(FIELDS):
                macc[n, i] += tot[n]
            for p in range(2):
                bacc[p, i] += kap * right[p]

    def z_ready(s):
        @pl.when(below)
        def _():
            from_below(s).wait_recv()

        @pl.when(above)
        def _():
            from_above(s).wait_recv()

    for k in order:
        s = lax.rem(f - k + nf, nf)
        arrivals(s)[1].wait_recv()
        forwards(s)

    z_ready(f)
    group(f)

    def step(k, carry):
        s = lax.rem(f - k + nf, nf)
        arrivals(s)[0].wait_recv()
        z_ready(s)
        group(s)
        return carry

    lax.fori_loop(1, nf, step, 0)

    for i in range(depth):
        for p in range(2):
            gath[0, f, p, i] = -bacc[p, i]

    def plane_sends(t):
        own = gath.at[t, f]
        return ((above, remote(own.at[:, depth - 1], mlo.at[t], pl_s.at[t, 0], pl_r.at[t, 0], f, zn)),
                (below, remote(own.at[:, 0], mhi.at[t], pl_s.at[t, 1], pl_r.at[t, 1], f, zp)),
                (diag_up, remote(own.at[:, depth - 1], mloc.at[t], pl_s.at[t, 2], pl_r.at[t, 2], f - 1, zn)),
                (diag_down, remote(own.at[:, 0], mhic.at[t], pl_s.at[t, 3], pl_r.at[t, 3], f + 1, zp)))

    def plane_arrivals(t):
        own = gath.at[t, f]
        return ((below, remote(own.at[:, depth - 1], mlo.at[t], pl_s.at[t, 0], pl_r.at[t, 0], f, zp)),
                (above, remote(own.at[:, 0], mhi.at[t], pl_s.at[t, 1], pl_r.at[t, 1], f, zn)),
                (diag_down, remote(own.at[:, depth - 1], mloc.at[t], pl_s.at[t, 2], pl_r.at[t, 2], f + 1, zp)),
                (diag_up, remote(own.at[:, 0], mhic.at[t], pl_s.at[t, 3], pl_r.at[t, 3], f - 1, zn)))

    def started(pairs):
        for cond, copy in pairs:
            pl.when(cond)(copy.start)

    def received(pairs):
        for cond, copy in pairs:
            pl.when(cond)(copy.wait_recv)

    def sent(pairs):
        for cond, copy in pairs:
            pl.when(cond)(copy.wait_send)

    def tile_send(t, k):
        return remote(gath.at[t, f], gath.at[t, f], ag_s.at[t, k], ag_r.at[t, f], lax.rem(f + k, nf), z)

    def tile_from(t, s):
        return remote(gath.at[t, s], gath.at[t, s], ag_s.at[t, 0], ag_r.at[t, s], s, z)

    started(plane_sends(0))
    for k in order[:2]:
        tile_send(0, k).start()

    y_first = jnp.logical_and(lax.broadcasted_iota(jnp.int32, (rows, width), 0) == 0, f == 0)
    for i in range(depth):
        w = weight(i)
        zm = w * jnp.where(below, 1.0, 0.0).astype(jnp.float32) if i == 0 else w
        for n in range(FIELDS):
            val = macc[n, i] * (zm if n < YY else w)
            if n in (YY, Y0, Y0 + 1, YX, YX + 1, ZY, ZY + 1):
                val = jnp.where(y_first, 0.0, val)
            if n in (XX, ZX, ZX + 1, YX, YX + 1, C0X, C0X + 1):
                val = jnp.where(lane_first, 0.0, val)
            macc[n, i] = val
            if n in (ZY, ZY + 1):
                ysrc[5 + n - ZY, i:i + 1, :] = val[0:1]
            elif YY <= n < CC:
                ysrc[n - YY, i:i + 1, :] = val[0:1]

    mz_pair = ((below, remote(macc.at[0:YY, 0], mz, mz_sem.at[0], mz_sem.at[1], f, zp)),)
    mz_from = ((above, remote(macc.at[0:YY, 0], mz, mz_sem.at[0], mz_sem.at[1], f, zn)),)
    yp_pair = ((first, remote(ysrc, yp, yp_sem.at[0], yp_sem.at[1], fprev, z)),)
    yp_from = ((last, remote(ysrc, yp, yp_sem.at[0], yp_sem.at[1], fnext, z)),)
    started(mz_pair)
    started(yp_pair)
    for k in order[2:]:
        tile_send(0, k).start()

    def apply(t):
        rows_next = [gath[t, fnext, p, :, 0, :] for p in range(2)]
        rows_here = [gath[t, f, p, :, rows - 1, :] for p in range(2)]
        rows_z = [jnp.concatenate([mloc[t, p, 0:1, :], rows_next[p][:-1]], axis=0) for p in range(2)]
        rows_x = [lane_prev(rows_next[p]) for p in range(2)]
        vy_edge = add(scale(yp[0], rows_here), mul((yp[1], yp[2]), rows_next), mul((yp[3], yp[4]), rows_x),
                      cmul((yp[5], yp[6]), rows_z))
        m4 = [mhi[t, p] for p in range(2)]
        m4y = [shifted_down(m4[p], mhic[t, p, rows - 1:rows, :]) for p in range(2)]
        m4x = [lane_prev(m4[p]) for p in range(2)]
        m4z = [gath[t, f, p, depth - 1] for p in range(2)]
        vz_edge = add(scale(mz[ZZ], m4z), mul((mz[Z0], mz[Z0 + 1]), m4), mul((mz[ZY], mz[ZY + 1]), m4y),
                      mul((mz[ZX], mz[ZX + 1]), m4x))
        after = vz_edge
        for i in reversed(range(depth)):
            m = [gath[t, f, p, i] for p in range(2)]
            m_z = [gath[t, f, p, i - 1] if i > 0 else mlo[t, p] for p in range(2)]
            m_y = [shifted_down(m[p], gath[t, fprev, p, i, rows - 1:rows, :]) for p in range(2)]
            m_x = [lane_prev(m[p]) for p in range(2)]

            def pair(n):
                return macc[n, i], macc[n + 1, i]

            z0, zy, zx, y0, yx, cx = pair(Z0), pair(ZY), pair(ZX), pair(Y0), pair(YX), pair(C0X)
            v0 = add(scale(macc[CC, i], m), cmul(z0, m_z), cmul(y0, m_y), mul(cx, m_x))
            vx = add(scale(macc[XX, i], m_x), cmul(cx, m), cmul(zx, m_z), cmul(yx, m_y))
            vy = add(scale(macc[YY, i], m_y), mul(y0, m), mul(yx, m_x), cmul(zy, m_z))
            vz = add(scale(macc[ZZ, i], m_z), mul(z0, m), mul(zy, m_y), mul(zx, m_x))
            for p in range(2):
                gath[t + 1, f, p, i] = (v0[p] + lane_next(vx[p]) + shifted_up(vy[p], vy_edge[p][i:i + 1])
                                        + after[p] + DAMPING * m[p])
            after = vz

    def halo_ready(t):
        received(plane_arrivals(t))
        tile_from(t, fnext).wait_recv()
        tile_from(t, fprev).wait_recv()

    received(mz_from)
    received(yp_from)
    halo_ready(0)
    apply(0)

    def exchange_over_freq(n, values):
        for row, value in enumerate(values):
            scs[n, row:row + 1, :] = jnp.sum(value, axis=0, keepdims=True)
        for k in order:
            part_send(n, k).start()

    def exchange_over_gz(n):
        total = scs[n]
        for k in order:
            s = lax.rem(f - k + nf, nf)
            remote(scs.at[n], scr.at[n, s], sc_s.at[n, k], sc_r.at[n, s], s, z).wait_recv()
            total = total + scr[n, s]
        sgs[n] = total
        for k in range(1, nz):
            sum_send(n, k).start()

    def exchanged(n):
        total = sgs[n]
        for k in range(1, nz):
            s = lax.rem(z - k + nz, nz)
            remote(sgs.at[n], sgr.at[n, s], sg_s.at[n, k], sg_r.at[n, s], f, s).wait_recv()
            total = total + sgr[n, s]
        sums = jnp.sum(total, axis=1, keepdims=True)
        return [sums[row:row + 1, :] for row in range(4)]

    def part_send(n, k):
        return remote(scs.at[n], scr.at[n, f], sc_s.at[n, k], sc_r.at[n, f], lax.rem(f + k, nf), z)

    def sum_send(n, k):
        return remote(sgs.at[n], sgr.at[n, z], sg_s.at[n, k], sg_r.at[n, z], f, lax.rem(z + k, nz))

    def inner(pairs):
        return sum(a * b for a, b in pairs)

    def tiles(t):
        return [gath[t, f, p, i] for p in range(2) for i in range(depth)]

    started(plane_sends(1))
    for k in order[:2]:
        tile_send(1, k).start()
    scs[...] = jnp.zeros_like(scs)
    right, image = tiles(0), tiles(1)
    exchange_over_freq(0, (inner(zip(right, right)), inner(zip(right, image))))
    for k in order[2:]:
        tile_send(1, k).start()
    exchange_over_gz(0)
    halo_ready(1)
    apply(1)
    bb, bq = exchanged(0)[:2]
    alpha = bb / bq
    step_size = jnp.broadcast_to(alpha, (rows, width))
    right, image = tiles(0), tiles(1)
    left = [b - step_size * q for b, q in zip(right, image)]
    exchange_over_freq(1, (inner(zip(left, left)), inner(zip(left, image)),
                           inner((r, q - step_size * s) for r, q, s in zip(left, image, tiles(2)))))
    for k in order:
        tile_send(2, k).start()
    exchange_over_gz(1)
    rr, rq, rnr = exchanged(1)[:3]
    ratio = rr / bb
    second = rr / (rnr + 2.0 * ratio * rq + ratio * ratio * bq)
    c1 = jnp.broadcast_to(alpha + second * (1.0 + ratio), (rows, width))
    c2 = jnp.broadcast_to(alpha * second, (rows, width))

    def finish(s):
        for p in range(2):
            for i in range(depth):
                b, q, r = gath[0, s, p, i], gath[1, s, p, i], gath[2, s, p, i]
                mod_out[p, i, s] = c1 * b - c2 * q
                res_out[p, i, s] = b - c1 * q + c2 * r

    finish(f)
    for k in order:
        s = lax.rem(f - k + nf, nf)
        if k not in (1, nf - 1):
            tile_from(0, s).wait_recv()
            tile_from(1, s).wait_recv()
        tile_from(2, s).wait_recv()
        finish(s)

    for k in range(1, nf):
        for copy in sends(lax.rem(f + k, nf)):
            copy.wait_send()
        for t in range(3):
            tile_send(t, k).wait_send()
        for n in range(2):
            part_send(n, k).wait_send()
    for s in range(nf):
        pl.when(above)(forward_up(s).wait_send)
        pl.when(below)(forward_down(s).wait_send)
    pl.when(below)(w_copy.wait_send)
    sent(mz_pair)
    sent(yp_pair)
    for t in range(2):
        sent(plane_sends(t))
    for k in range(1, nz):
        for n in range(2):
            sum_send(n, k).wait_send()


def body(nf, nz, displacement, freq_index, tissue):
    _, _, comps, depth, height, width = displacement.shape
    rows = height // nf
    u = displacement.reshape(2, comps, depth, nf, rows, width)
    tis = tissue.reshape(depth, nf, rows, width)
    f32 = jnp.float32
    dma = pltpu.SemaphoreType.DMA
    vmem = pl.BlockSpec(memory_space=pltpu.VMEM)
    out = jax.ShapeDtypeStruct((2, depth, nf, rows, width), f32)
    modulus, residual = pl.pallas_call(
        functools.partial(kernel, nf, nz),
        out_shape=(out, out),
        in_specs=[vmem, vmem, pl.BlockSpec(memory_space=pltpu.SMEM)],
        out_specs=(vmem, vmem),
        scratch_shapes=[
            pltpu.VMEM((nf, 2, comps, depth, rows, width), f32),
            pltpu.VMEM((nf, 2 * comps + 1, 2 * depth, width), f32),
            pltpu.VMEM((nf, 2 * comps + 1, 2 * depth, width), f32),
            pltpu.VMEM((nf, 2, comps, rows, width), f32),
            pltpu.VMEM((nf, 2, comps, rows, width), f32),
            pltpu.VMEM((rows, width), f32),
            pltpu.VMEM((rows, width), f32),
            pltpu.VMEM((FIELDS, depth, rows, width), f32),
            pltpu.VMEM((2, depth, rows, width), f32),
            pltpu.VMEM((YY, rows, width), f32),
            pltpu.VMEM((7, depth, width), f32),
            pltpu.VMEM((7, depth, width), f32),
            pltpu.VMEM((3, nf, 2, depth, rows, width), f32),
            pltpu.VMEM((2, 2, rows, width), f32),
            pltpu.VMEM((2, 2, rows, width), f32),
            pltpu.VMEM((2, 2, rows, width), f32),
            pltpu.VMEM((2, 2, rows, width), f32),
            pltpu.VMEM((2, 4, width), f32),
            pltpu.VMEM((2, nf, 4, width), f32),
            pltpu.VMEM((2, 4, width), f32),
            pltpu.VMEM((2, nz, 4, width), f32),
            dma((2,)), dma((nf,)), dma((nf,)), dma((nf,)), dma((nf,)),
            dma((nf,)), dma((nf,)), dma((nf,)), dma((nf,)),
            dma((2,)), dma((2,)), dma((2,)),
            dma((3, nf)), dma((3, nf)), dma((2, 4)), dma((2, 4)),
            dma((2, nf)), dma((2, nf)), dma((2, nz)), dma((2, nz)),
        ],
        compiler_params=pltpu.CompilerParams(collective_id=0, has_side_effects=True),
    )(u, tis, freq_index)
    shape = (2, depth, height, width)
    return modulus.reshape(shape), residual.reshape(shape)


def solution(mesh):
    placed = (P("freq", None, None, "gz", None, None), P("freq"), P("gz", None, None))
    return jax.shard_map(
        functools.partial(body, mesh.shape["freq"], mesh.shape["gz"]),
        mesh=mesh,
        in_specs=placed,
        out_specs=(P(None, "gz", None, None), P(None, "gz", None, None)),
        check_vma=False,
    )
```

```python
import functools

import jax
import jax.numpy as jnp
from jax import lax
from jax.experimental import pallas as pl
from jax.experimental.pallas import tpu as pltpu
from jax.sharding import PartitionSpec as P

MESH = pl.DeviceIdType.MESH
DAMPING = 0.05
ZZ, Z0, ZY, ZX = 0, 1, 3, 5
YY, Y0, YX = 7, 8, 10
CC, C0X, XX = 12, 13, 15
FIELDS = 16


def shifted_up(array, tail):
    rows = array.shape[0]
    if rows % 8 == 0:
        last = lax.broadcasted_iota(jnp.int32, array.shape, 0) == rows - 1
        return jnp.where(last, jnp.broadcast_to(tail, array.shape), pltpu.roll(array, rows - 1, 0))
    return jnp.concatenate([array[1:], tail], axis=0)


def shifted_down(array, head):
    rows = array.shape[0]
    if rows % 8 == 0:
        first = lax.broadcasted_iota(jnp.int32, array.shape, 0) == 0
        return jnp.where(first, jnp.broadcast_to(head, array.shape), pltpu.roll(array, 1, 0))
    return jnp.concatenate([head, array[:-1]], axis=0)


def lane_next(array):
    return pltpu.roll(array, array.shape[1] - 1, 1)


def lane_prev(array):
    return pltpu.roll(array, 1, 1)


def mul(a, b):
    return a[0] * b[0] - a[1] * b[1], a[0] * b[1] + a[1] * b[0]


def cmul(a, b):
    return a[0] * b[0] + a[1] * b[1], a[0] * b[1] - a[1] * b[0]


def add(*terms):
    return sum(t[0] for t in terms[1:]) + terms[0][0], sum(t[1] for t in terms[1:]) + terms[0][1]


def scale(r, a):
    return r * a[0], r * a[1]


def kernel(nf, nz, u, tis, fi, mod_out, res_out,
           ubuf, hsrc, hbuf, zlo, zhi, wsrc, wz, macc, bacc, mz, ysrc, yp, gath, mlo, mloc, mhi, mhic,
           scs, scr, sgs, sgr,
           loc_s, main_s, main_r, halo_s, halo_r, flo_s, fhi_s, zlo_r, zhi_r, w_sem, mz_sem, yp_sem,
           ag_s, ag_r, pl_s, pl_r, sc_s, sc_r, sg_s, sg_r):
    f = lax.axis_index("freq")
    z = lax.axis_index("gz")
    _, comps, depth, _, rows, width = u.shape
    below, above = z > 0, z < nz - 1
    first, last = f > 0, f < nf - 1
    fnext, fprev = lax.rem(f + 1, nf), lax.rem(f + nf - 1, nf)
    zn, zp = z + 1, z - 1

    def remote(src, dst, ssem, rsem, df, dz):
        return pltpu.make_async_remote_copy(
            src_ref=src, dst_ref=dst, send_sem=ssem, recv_sem=rsem, device_id=(df, dz), device_id_type=MESH)

    barrier = pltpu.get_barrier_semaphore()

    def greet(df, dz):
        pl.semaphore_signal(barrier, inc=1, device_id=(df, dz), device_id_type=MESH)

    for k in range(1, nf):
        greet(lax.rem(f + k, nf), z)
    for k in range(1, nz):
        greet(f, lax.rem(z + k, nz))
    diag_up = jnp.logical_and(first, above)
    diag_down = jnp.logical_and(last, below)

    @pl.when(diag_up)
    def _():
        greet(f - 1, zn)

    @pl.when(diag_down)
    def _():
        greet(f + 1, zp)

    kappa = 0.2 * (fi[0] + 1).astype(jnp.float32)
    zero_row = jnp.zeros((1, width), jnp.float32)
    for d in range(nf):
        for p in range(2):
            for c in range(comps):
                for i in range(depth):
                    lo = u[p, c, i, d - 1, rows - 1:rows, :] if d > 0 else zero_row
                    hi = u[p, c, i, d + 1, 0:1, :] if d < nf - 1 else zero_row
                    hsrc[d, p * comps + c, i:i + 1, :] = lo
                    hsrc[d, p * comps + c, depth + i:depth + i + 1, :] = hi
        hsrc[d, 2 * comps] = jnp.full((2 * depth, width), kappa, jnp.float32)
    wsrc[...] = tis[0, f].astype(jnp.float32)

    @pl.when(jnp.logical_not(below))
    def _():
        zlo[...] = jnp.zeros_like(zlo)
        mlo[...] = jnp.zeros_like(mlo)

    @pl.when(jnp.logical_not(above))
    def _():
        zhi[...] = jnp.zeros_like(zhi)
        mhi[...] = jnp.zeros_like(mhi)
        wz[...] = jnp.zeros_like(wz)
        mz[...] = jnp.zeros_like(mz)

    @pl.when(jnp.logical_not(last))
    def _():
        yp[...] = jnp.zeros_like(yp)

    @pl.when(jnp.logical_not(diag_up))
    def _():
        mhic[...] = jnp.zeros_like(mhic)

    @pl.when(jnp.logical_not(diag_down))
    def _():
        mloc[...] = jnp.zeros_like(mloc)

    own_u = pltpu.make_async_copy(u.at[:, :, :, f], ubuf.at[f], loc_s.at[0])
    own_h = pltpu.make_async_copy(hsrc.at[f], hbuf.at[f], loc_s.at[1])
    own_u.start()
    own_h.start()
    macc[...] = jnp.zeros_like(macc)
    bacc[...] = jnp.zeros_like(bacc)

    pl.semaphore_wait(barrier, (nf - 1) + (nz - 1) + diag_up.astype(jnp.int32) + diag_down.astype(jnp.int32))

    order = []
    for k in range(1, nf // 2 + 1):
        order.append(k)
        if nf - k != k:
            order.append(nf - k)

    def sends(d):
        return (remote(hsrc.at[d], hbuf.at[f], halo_s.at[d], halo_r.at[f], d, z),
                remote(u.at[:, :, :, d], ubuf.at[f], main_s.at[d], main_r.at[f], d, z))

    def arrivals(s):
        return (remote(hsrc.at[s], hbuf.at[s], halo_s.at[s], halo_r.at[s], s, z),
                remote(u.at[:, :, :, s], ubuf.at[s], main_s.at[s], main_r.at[s], s, z))

    for part in (1, 0):
        for k in order:
            sends(lax.rem(f + k, nf))[part].start()

    w_copy = remote(wsrc, wz, w_sem.at[0], w_sem.at[1], f, zp)
    w_from = remote(wsrc, wz, w_sem.at[0], w_sem.at[1], f, zn)

    @pl.when(below)
    def _():
        w_copy.start()

    def forward_up(s):
        return remote(ubuf.at[s, :, :, depth - 1], zlo.at[s], flo_s.at[s], zlo_r.at[s], f, zn)

    def forward_down(s):
        return remote(ubuf.at[s, :, :, 0], zhi.at[s], fhi_s.at[s], zhi_r.at[s], f, zp)

    def from_below(s):
        return remote(ubuf.at[s, :, :, depth - 1], zlo.at[s], flo_s.at[s], zlo_r.at[s], f, zp)

    def from_above(s):
        return remote(ubuf.at[s, :, :, 0], zhi.at[s], fhi_s.at[s], zhi_r.at[s], f, zn)

    def forwards(s):
        @pl.when(above)
        def _():
            forward_up(s).start()

        @pl.when(below)
        def _():
            forward_down(s).start()

    own_u.wait()
    own_h.wait()
    forwards(f)

    @pl.when(above)
    def _():
        w_from.wait_recv()

    lane_last = lax.broadcasted_iota(jnp.int32, (rows, width), 1) == width - 1
    lane_first = lax.broadcasted_iota(jnp.int32, (rows, width), 1) == 0
    last_scale = jnp.where(last, 1.0, 0.0).astype(jnp.float32)

    def weight(i):
        return tis[i, f].astype(jnp.float32)

    def group(s):
        kap = hbuf[s, 2 * comps, 0:1, :]
        for i in range(depth):
            w = weight(i)
            w_z = weight(i + 1) if i + 1 < depth else wz[...]
            w_y = shifted_up(w, tis[i, fnext, 0:1, :].astype(jnp.float32) * last_scale)
            w_x = jnp.where(lane_last, 0.0, lane_next(w))
            tot = [None] * FIELDS
            right = None
            for c in range(comps):
                here, az, ay, ax, gz, gy, gx, uz, uy, ux = ([None, None] for _ in range(10))
                for p in range(2):
                    v = ubuf[s, p, c, i]
                    prev_z = ubuf[s, p, c, i - 1] if i > 0 else zlo[s, p, c]
                    next_z = ubuf[s, p, c, i + 1] if i + 1 < depth else zhi[s, p, c]
                    lo = hbuf[s, p * comps + c, i:i + 1, :]
                    hi = hbuf[s, p * comps + c, depth + i:depth + i + 1, :]
                    next_y = shifted_up(v, hi)
                    prev_y = shifted_down(v, lo)
                    next_x = jnp.where(lane_last, 0.0, lane_next(v))
                    prev_x = lane_prev(v)
                    here[p] = v
                    uz[p], uy[p], ux[p] = next_z, next_y, next_x
                    gz[p], gy[p], gx[p] = next_z - v, next_y - v, next_x - v
                    az[p], ay[p], ax[p] = v - prev_z, v - prev_y, v - prev_x
                h = [-(gz[p] + gy[p] + gx[p]) for p in range(2)]
                parts = [None] * FIELDS
                parts[ZZ] = az[0] * az[0] + az[1] * az[1]
                parts[YY] = ay[0] * ay[0] + ay[1] * ay[1]
                parts[XX] = ax[0] * ax[0] + ax[1] * ax[1]
                parts[CC] = h[0] * h[0] + h[1] * h[1]
                parts[Z0:Z0 + 2] = cmul(az, h)
                parts[ZY:ZY + 2] = cmul(az, ay)
                parts[ZX:ZX + 2] = cmul(az, ax)
                parts[Y0:Y0 + 2] = cmul(ay, h)
                parts[YX:YX + 2] = cmul(ay, ax)
                parts[C0X:C0X + 2] = cmul(h, ax)
                tot = parts if c == 0 else [a + b for a, b in zip(tot, parts)]
                t = [w * here[p] for p in range(2)]
                for g, wn, un in ((gz, w_z, uz), (gy, w_y, uy), (gx, w_x, ux)):
                    term = cmul(g, [t[p] - wn * un[p] for p in range(2)])
                    right = term if right is None else add(right, term)
            for n in range(FIELDS):
                macc[n, i] += tot[n]
            for p in range(2):
                bacc[p, i] += kap * right[p]

    def z_ready(s):
        @pl.when(below)
        def _():
            from_below(s).wait_recv()

        @pl.when(above)
        def _():
            from_above(s).wait_recv()

    for k in order:
        s = lax.rem(f - k + nf, nf)
        arrivals(s)[1].wait_recv()
        forwards(s)

    z_ready(f)
    group(f)

    def step(k, carry):
        s = lax.rem(f - k + nf, nf)
        arrivals(s)[0].wait_recv()
        z_ready(s)
        group(s)
        return carry

    lax.fori_loop(1, nf, step, 0)

    for i in range(depth):
        for p in range(2):
            gath[0, f, p, i] = -bacc[p, i]

    def plane_sends(t):
        own = gath.at[t, f]
        return ((above, remote(own.at[:, depth - 1], mlo.at[t], pl_s.at[t, 0], pl_r.at[t, 0], f, zn)),
                (below, remote(own.at[:, 0], mhi.at[t], pl_s.at[t, 1], pl_r.at[t, 1], f, zp)),
                (diag_up, remote(own.at[:, depth - 1], mloc.at[t], pl_s.at[t, 2], pl_r.at[t, 2], f - 1, zn)),
                (diag_down, remote(own.at[:, 0], mhic.at[t], pl_s.at[t, 3], pl_r.at[t, 3], f + 1, zp)))

    def plane_arrivals(t):
        own = gath.at[t, f]
        return ((below, remote(own.at[:, depth - 1], mlo.at[t], pl_s.at[t, 0], pl_r.at[t, 0], f, zp)),
                (above, remote(own.at[:, 0], mhi.at[t], pl_s.at[t, 1], pl_r.at[t, 1], f, zn)),
                (diag_down, remote(own.at[:, depth - 1], mloc.at[t], pl_s.at[t, 2], pl_r.at[t, 2], f + 1, zp)),
                (diag_up, remote(own.at[:, 0], mhic.at[t], pl_s.at[t, 3], pl_r.at[t, 3], f - 1, zn)))

    def started(pairs):
        for cond, copy in pairs:
            pl.when(cond)(copy.start)

    def received(pairs):
        for cond, copy in pairs:
            pl.when(cond)(copy.wait_recv)

    def sent(pairs):
        for cond, copy in pairs:
            pl.when(cond)(copy.wait_send)

    def tile_send(t, k):
        return remote(gath.at[t, f], gath.at[t, f], ag_s.at[t, k], ag_r.at[t, f], lax.rem(f + k, nf), z)

    def tile_from(t, s):
        return remote(gath.at[t, s], gath.at[t, s], ag_s.at[t, 0], ag_r.at[t, s], s, z)

    started(plane_sends(0))
    for k in order[:2]:
        tile_send(0, k).start()

    y_first = jnp.logical_and(lax.broadcasted_iota(jnp.int32, (rows, width), 0) == 0, f == 0)
    for i in range(depth):
        w = weight(i)
        zm = w * jnp.where(below, 1.0, 0.0).astype(jnp.float32) if i == 0 else w
        for n in range(FIELDS):
            val = macc[n, i] * (zm if n < YY else w)
            if n in (YY, Y0, Y0 + 1, YX, YX + 1, ZY, ZY + 1):
                val = jnp.where(y_first, 0.0, val)
            if n in (XX, ZX, ZX + 1, YX, YX + 1, C0X, C0X + 1):
                val = jnp.where(lane_first, 0.0, val)
            macc[n, i] = val
            if n in (ZY, ZY + 1):
                ysrc[5 + n - ZY, i:i + 1, :] = val[0:1]
            elif YY <= n < CC:
                ysrc[n - YY, i:i + 1, :] = val[0:1]

    mz_pair = ((below, remote(macc.at[0:YY, 0], mz, mz_sem.at[0], mz_sem.at[1], f, zp)),)
    mz_from = ((above, remote(macc.at[0:YY, 0], mz, mz_sem.at[0], mz_sem.at[1], f, zn)),)
    yp_pair = ((first, remote(ysrc, yp, yp_sem.at[0], yp_sem.at[1], fprev, z)),)
    yp_from = ((last, remote(ysrc, yp, yp_sem.at[0], yp_sem.at[1], fnext, z)),)
    started(mz_pair)
    started(yp_pair)
    for k in order[2:]:
        tile_send(0, k).start()

    def apply(t):
        rows_next = [gath[t, fnext, p, :, 0, :] for p in range(2)]
        rows_here = [gath[t, f, p, :, rows - 1, :] for p in range(2)]
        rows_z = [jnp.concatenate([mloc[t, p, 0:1, :], rows_next[p][:-1]], axis=0) for p in range(2)]
        rows_x = [lane_prev(rows_next[p]) for p in range(2)]
        vy_edge = add(scale(yp[0], rows_here), mul((yp[1], yp[2]), rows_next), mul((yp[3], yp[4]), rows_x),
                      cmul((yp[5], yp[6]), rows_z))
        m4 = [mhi[t, p] for p in range(2)]
        m4y = [shifted_down(m4[p], mhic[t, p, rows - 1:rows, :]) for p in range(2)]
        m4x = [lane_prev(m4[p]) for p in range(2)]
        m4z = [gath[t, f, p, depth - 1] for p in range(2)]
        vz_edge = add(scale(mz[ZZ], m4z), mul((mz[Z0], mz[Z0 + 1]), m4), mul((mz[ZY], mz[ZY + 1]), m4y),
                      mul((mz[ZX], mz[ZX + 1]), m4x))
        after = vz_edge
        for i in reversed(range(depth)):
            m = [gath[t, f, p, i] for p in range(2)]
            m_z = [gath[t, f, p, i - 1] if i > 0 else mlo[t, p] for p in range(2)]
            m_y = [shifted_down(m[p], gath[t, fprev, p, i, rows - 1:rows, :]) for p in range(2)]
            m_x = [lane_prev(m[p]) for p in range(2)]

            def pair(n):
                return macc[n, i], macc[n + 1, i]

            z0, zy, zx, y0, yx, cx = pair(Z0), pair(ZY), pair(ZX), pair(Y0), pair(YX), pair(C0X)
            v0 = add(scale(macc[CC, i], m), cmul(z0, m_z), cmul(y0, m_y), mul(cx, m_x))
            vx = add(scale(macc[XX, i], m_x), cmul(cx, m), cmul(zx, m_z), cmul(yx, m_y))
            vy = add(scale(macc[YY, i], m_y), mul(y0, m), mul(yx, m_x), cmul(zy, m_z))
            vz = add(scale(macc[ZZ, i], m_z), mul(z0, m), mul(zy, m_y), mul(zx, m_x))
            for p in range(2):
                gath[t + 1, f, p, i] = (v0[p] + lane_next(vx[p]) + shifted_up(vy[p], vy_edge[p][i:i + 1])
                                        + after[p] + DAMPING * m[p])
            after = vz

    def halo_ready(t):
        received(plane_arrivals(t))
        tile_from(t, fnext).wait_recv()
        tile_from(t, fprev).wait_recv()

    received(mz_from)
    received(yp_from)
    halo_ready(0)
    apply(0)

    def exchange_over_freq(n, values):
        for row, value in enumerate(values):
            scs[n, row:row + 1, :] = jnp.sum(value, axis=0, keepdims=True)
        for k in order:
            part_send(n, k).start()

    def exchange_over_gz(n):
        total = scs[n]
        for k in order:
            s = lax.rem(f - k + nf, nf)
            remote(scs.at[n], scr.at[n, s], sc_s.at[n, k], sc_r.at[n, s], s, z).wait_recv()
            total = total + scr[n, s]
        sgs[n] = total
        for k in range(1, nz):
            sum_send(n, k).start()

    def exchanged(n):
        total = sgs[n]
        for k in range(1, nz):
            s = lax.rem(z - k + nz, nz)
            remote(sgs.at[n], sgr.at[n, s], sg_s.at[n, k], sg_r.at[n, s], f, s).wait_recv()
            total = total + sgr[n, s]
        sums = jnp.sum(total, axis=1, keepdims=True)
        return [sums[row:row + 1, :] for row in range(4)]

    def part_send(n, k):
        return remote(scs.at[n], scr.at[n, f], sc_s.at[n, k], sc_r.at[n, f], lax.rem(f + k, nf), z)

    def sum_send(n, k):
        return remote(sgs.at[n], sgr.at[n, z], sg_s.at[n, k], sg_r.at[n, z], f, lax.rem(z + k, nz))

    def inner(pairs):
        return sum(a * b for a, b in pairs)

    def tiles(t):
        return [gath[t, f, p, i] for p in range(2) for i in range(depth)]

    started(plane_sends(1))
    for k in order:
        tile_send(1, k).start()
    right, image = tiles(0), tiles(1)
    moments = [inner(zip(right, right)), inner(zip(right, image)), inner(zip(image, image))]
    halo_ready(1)
    apply(1)
    exchange_over_freq(0, moments + [inner(zip(image, tiles(2)))])
    for k in order:
        tile_send(2, k).start()
    exchange_over_gz(0)
    bb, bq, qq, qs = exchanged(0)
    alpha = bb / bq
    norm = bb - 2.0 * alpha * bq + alpha * alpha * qq
    beta = 1.0 + norm / bb
    second = norm / (beta * beta * bq - 2.0 * alpha * beta * qq + alpha * alpha * qs)
    c1 = jnp.broadcast_to(alpha + second * beta, (rows, width))
    c2 = jnp.broadcast_to(alpha * second, (rows, width))

    def finish(s):
        for p in range(2):
            for i in range(depth):
                b, q, r = gath[0, s, p, i], gath[1, s, p, i], gath[2, s, p, i]
                mod_out[p, i, s] = c1 * b - c2 * q
                res_out[p, i, s] = b - c1 * q + c2 * r

    finish(f)
    for k in order:
        s = lax.rem(f - k + nf, nf)
        if k not in (1, nf - 1):
            tile_from(0, s).wait_recv()
            tile_from(1, s).wait_recv()
        tile_from(2, s).wait_recv()
        finish(s)

    for k in range(1, nf):
        for copy in sends(lax.rem(f + k, nf)):
            copy.wait_send()
        for t in range(3):
            tile_send(t, k).wait_send()
        part_send(0, k).wait_send()
    for s in range(nf):
        pl.when(above)(forward_up(s).wait_send)
        pl.when(below)(forward_down(s).wait_send)
    pl.when(below)(w_copy.wait_send)
    sent(mz_pair)
    sent(yp_pair)
    for t in range(2):
        sent(plane_sends(t))
    for k in range(1, nz):
        sum_send(0, k).wait_send()


def body(nf, nz, displacement, freq_index, tissue):
    _, _, comps, depth, height, width = displacement.shape
    rows = height // nf
    u = displacement.reshape(2, comps, depth, nf, rows, width)
    tis = tissue.reshape(depth, nf, rows, width)
    f32 = jnp.float32
    dma = pltpu.SemaphoreType.DMA
    vmem = pl.BlockSpec(memory_space=pltpu.VMEM)
    out = jax.ShapeDtypeStruct((2, depth, nf, rows, width), f32)
    modulus, residual = pl.pallas_call(
        functools.partial(kernel, nf, nz),
        out_shape=(out, out),
        in_specs=[vmem, vmem, pl.BlockSpec(memory_space=pltpu.SMEM)],
        out_specs=(vmem, vmem),
        scratch_shapes=[
            pltpu.VMEM((nf, 2, comps, depth, rows, width), f32),
            pltpu.VMEM((nf, 2 * comps + 1, 2 * depth, width), f32),
            pltpu.VMEM((nf, 2 * comps + 1, 2 * depth, width), f32),
            pltpu.VMEM((nf, 2, comps, rows, width), f32),
            pltpu.VMEM((nf, 2, comps, rows, width), f32),
            pltpu.VMEM((rows, width), f32),
            pltpu.VMEM((rows, width), f32),
            pltpu.VMEM((FIELDS, depth, rows, width), f32),
            pltpu.VMEM((2, depth, rows, width), f32),
            pltpu.VMEM((YY, rows, width), f32),
            pltpu.VMEM((7, depth, width), f32),
            pltpu.VMEM((7, depth, width), f32),
            pltpu.VMEM((3, nf, 2, depth, rows, width), f32),
            pltpu.VMEM((2, 2, rows, width), f32),
            pltpu.VMEM((2, 2, rows, width), f32),
            pltpu.VMEM((2, 2, rows, width), f32),
            pltpu.VMEM((2, 2, rows, width), f32),
            pltpu.VMEM((2, 4, width), f32),
            pltpu.VMEM((2, nf, 4, width), f32),
            pltpu.VMEM((2, 4, width), f32),
            pltpu.VMEM((2, nz, 4, width), f32),
            dma((2,)), dma((nf,)), dma((nf,)), dma((nf,)), dma((nf,)),
            dma((nf,)), dma((nf,)), dma((nf,)), dma((nf,)),
            dma((2,)), dma((2,)), dma((2,)),
            dma((3, nf)), dma((3, nf)), dma((2, 4)), dma((2, 4)),
            dma((2, nf)), dma((2, nf)), dma((2, nz)), dma((2, nz)),
        ],
        compiler_params=pltpu.CompilerParams(collective_id=0, has_side_effects=True),
    )(u, tis, freq_index)
    shape = (2, depth, height, width)
    return modulus.reshape(shape), residual.reshape(shape)


def solution(mesh):
    placed = (P("freq", None, None, "gz", None, None), P("freq"), P("gz", None, None))
    return jax.shard_map(
        functools.partial(body, mesh.shape["freq"], mesh.shape["gz"]),
        mesh=mesh,
        in_specs=placed,
        out_specs=(P(None, "gz", None, None), P(None, "gz", None, None)),
        check_vma=False,
    )
```
